32 devices in a mesh: rows: 8 (over z, x), grp: 4 (over y, core).
Axes of the slice: x: 2, y: 2, z: 4, core: 2. Of those that a mesh axis runs over, the one named last changes fastest.
Arguments:
- tile_values: bfloat16 [1024, 16, 128], P('rows'), may hold values from 0.049804688 to 1
- tile_ids: int32 [1024, 16], P('rows'), may hold values from 0 to 255, as said below
- doc_tiles: int32 [1024], P('rows'), may hold values from 1 to 16
- row_counts: int32 [8], replicated, may hold values from 1 to 128, 512 in all
Outputs:
- similarity: float32 [512, 512], P('rows', 'grp')
The draws below stay inside these ranges and needn't reach their ends.
Inputs may be any that keep to these rules, and one draw needn't show every extreme that they name: `row_counts`: the entries sum to 512. `tile_ids`: the 16 entries of a row are distinct.
All inputs are finite; a program needn't handle non-finite values.
Results may differ from the reference program's by a relative error of at most 0.0003.
Values may be sent and summed in bfloat16 or wider, within the bound.
A program may use at most 64 MiB of HBM per device.

```python
import math
import jax
import jax.numpy as jnp
import numpy as np
from jax import lax

VOCAB = 32768
TILE = 128
LTILES = 16
DOC_DEV = 64
PANELS = 8
CAP = 128
DOCS = 512
N_ROWS = 8


def draw_doc_tiles(key, part):
    first_key, second_key = jax.random.split(jax.random.fold_in(key, 11))
    first_draw = jax.random.randint(first_key, (PANELS * CAP,), 1, LTILES + 1)
    second_draw = jax.random.randint(second_key, (PANELS * CAP,), 1, LTILES + 1)
    return jnp.maximum(first_draw, second_draw).astype(jnp.int32)


def draw_tile_ids(key, part):
    tile_count = VOCAB // TILE
    noise = jax.random.randint(jax.random.fold_in(key, 23), (PANELS * CAP, tile_count), 0, 4096)
    tile_rank = jnp.arange(tile_count, dtype=jnp.int32)
    scores = noise * (tile_rank + 8) * tile_count + tile_rank
    order = jnp.argsort(scores, axis=1)
    return order[:, :LTILES].astype(jnp.int32)


def level_of(stream_key, dims, cuts, least, top_value):
    def one(dim, parts):
        steps = jax.random.uniform(jax.random.fold_in(jax.random.fold_in(stream_key, 6), dim), (parts,), jnp.float32, least / len(cuts), top_value / len(cuts))
        return jnp.repeat(jnp.exp(steps), dims[dim] // parts).reshape((-1,) + (1,) * (len(dims) - dim - 1))

    level = one(*cuts[0])
    for cut in cuts[1:]:
        level = level * one(*cut)
    return level


def length_profile(amount, total, most, lean):
    loads = [(1 << 20) // math.isqrt(grade ** lean) + 1 for grade in range(2, amount + 1)]
    spare, given = total - most - (amount - 1), [1] * (amount - 1)
    while spare > 0:
        movable = [i for i in range(amount - 1) if given[i] < most]
        whole, left = sum([loads[i] for i in movable]), spare
        for i in movable:
            addition = min(most - given[i], max(1, left * loads[i] // whole), spare)
            given[i] = given[i] + addition
            spare = spare - addition
    return np.array([most] + given)


def uneven_parts(key, number_of, total, most, skew):
    if number_of == 2:
        one = jax.random.randint(key, (), max(1, total - most), min(most, total - 1) + 1)
        return jnp.stack([one, total - one])
    tallies = jnp.asarray(length_profile(number_of, total, most, skew), jnp.int32)
    couples = (number_of - 1) // 2
    source_of, sink = tallies[1:1 + 2 * couples:2], tallies[2:2 + 2 * couples:2]
    room = jnp.minimum(source_of - 1, most - sink)
    shifted = jax.random.randint(jax.random.fold_in(key, 1), (couples,), 0, 1 << 20) % (room + 1)
    tallies = tallies.at[1:1 + 2 * couples:2].set(source_of - shifted).at[2:2 + 2 * couples:2].set(sink + shifted)
    return tallies[jax.random.permutation(jax.random.fold_in(key, 2), number_of)]


def setup_inputs(seed: int = 0) -> dict:
    streams_of = jax.random.split(jax.random.key(seed), 5)
    return {
        "tile_values": jnp.clip(jnp.exp(math.log(1.0) - 2.9996462 * jax.random.uniform(streams_of[0], (PANELS * CAP, LTILES, TILE), jnp.float32) ** level_of(streams_of[0], (PANELS * CAP, LTILES, TILE), ((0, 8),), -0.2, 0.2)), 0.049804688, 1.0).astype(jnp.bfloat16),
        "tile_ids": draw_tile_ids(jax.random.fold_in(streams_of[4], 71), 0),
        "doc_tiles": draw_doc_tiles(jax.random.fold_in(streams_of[4], 71), 0),
        "row_counts": uneven_parts(streams_of[3], PANELS, DOCS, CAP, 2).astype(jnp.int32),
    }


def reference(tile_values, tile_ids, doc_tiles, row_counts):
    capacity = tile_values.shape[0] // N_ROWS
    live_mask = jnp.arange(LTILES, dtype=jnp.int32)[None, :] < doc_tiles[:, None]
    masked = jnp.where(live_mask[:, :, None], tile_values, jnp.zeros_like(tile_values))
    run_ends = jnp.cumsum(row_counts).astype(jnp.int32)
    run_starts = (run_ends - row_counts).astype(jnp.int32)
    position = jnp.arange(DOCS, dtype=jnp.int32)
    global_ids = ((position % DOC_DEV) * N_ROWS + position // DOC_DEV).astype(jnp.int32)
    source = jnp.searchsorted(run_ends, global_ids, side="right").astype(jnp.int32)
    slot_rows = (source * capacity + (global_ids - run_starts[source])).astype(jnp.int32)
    values = masked[slot_rows]
    codes = tile_ids[slot_rows]
    holder = jnp.zeros((DOCS, VOCAB // TILE, TILE), values.dtype)
    holder = holder.at[jnp.arange(DOCS, dtype=jnp.int32)[:, None], codes].set(values)
    dense = holder.reshape(DOCS, VOCAB)
    widened = values.astype(jnp.float32)
    norms = jnp.sum(widened * widened, axis=(1, 2))

    def panel(panel_index):
        rows_here = lax.dynamic_slice_in_dim(dense, panel_index * DOC_DEV, DOC_DEV, 0)
        norms_here = lax.dynamic_slice_in_dim(norms, panel_index * DOC_DEV, DOC_DEV, 0)
        product = jnp.dot(rows_here, dense.T, preferred_element_type=jnp.float32)
        ratio = product / (norms_here[:, None] + norms[None, :] - product)
        order = ((panel_index - jnp.arange(N_ROWS, dtype=jnp.int32)) % N_ROWS).astype(jnp.int32)
        return ratio.reshape(DOC_DEV, N_ROWS, DOC_DEV)[:, order, :].reshape(DOC_DEV, DOCS)

    result = lax.map(panel, jnp.arange(N_ROWS, dtype=jnp.int32))
    return result.reshape(DOCS, DOCS)
```

```python
import functools

import jax
import jax.numpy as jnp
from jax import lax
from jax.experimental import pallas as pl
from jax.experimental.pallas import tpu as pltpu
from jax.sharding import PartitionSpec as P

MESH = pl.DeviceIdType.MESH
DOC_DEV = 64


def kernel(R, G, counts_ref, tiles_ref, vals_ref, idblk_ref, out_ref,
           staged, place, work, own, other, own_ids, other_ids,
           send_sem, recv_sem, local_sem, *inc):
    cap, K, T = vals_ref.shape
    C = staged.shape[1] - 1
    M = len(inc)
    span = M - 1
    pair = other.shape[0] // (K * DOC_DEV)
    width = pair * DOC_DEV
    me = lax.axis_index("rows")
    grp = lax.axis_index("grp")

    barrier = pltpu.get_barrier_semaphore()

    def greet(d, _):
        pl.semaphore_signal(barrier, inc=1, device_id=(lax.rem(me + d, R), grp),
                            device_id_type=MESH)
        return 0

    lax.fori_loop(1, R, greet, 0)

    def add_up(r, total):
        return total + jnp.where(r < me, counts_ref[r], 0)

    start = lax.fori_loop(0, R, add_up, jnp.int32(0), unroll=R <= 8)
    tile_line = lax.broadcasted_iota(jnp.int32, (K, T), 0)

    def stage(j, _):
        b = lax.rem(j + R - lax.rem(start, R), R)
        for a in range(C):
            s = jnp.minimum(a * R + b, cap - 1)
            block = vals_ref[s].astype(jnp.float32)
            block = jnp.where(tile_line < tiles_ref[s], block, 0.0)
            staged[j, a] = block.astype(staged.dtype)
        staged[j, C] = idblk_ref[b]
        return 0

    lax.fori_loop(0, R, stage, 0)
    pl.semaphore_wait(barrier, R - 1)

    def panel_of(row, m):
        distance = grp * span + m - 1 if m else 0
        return lax.rem(row + R - distance, R)

    def remote(m, d):
        row = lax.rem(me + d, R)
        return pltpu.make_async_remote_copy(
            src_ref=staged.at[panel_of(row, m)], dst_ref=inc[m].at[me],
            send_sem=send_sem.at[m], recv_sem=recv_sem.at[m],
            device_id=(row, grp), device_id_type=MESH)

    def send_all(m):
        def send(i, _):
            remote(m, i).start()
            return 0

        lax.fori_loop(1, R, send, 0)
        pltpu.make_async_copy(staged.at[panel_of(me, m)], inc[m].at[me],
                              local_sem.at[m]).start()

    def wait_all(m):
        pltpu.make_async_copy(staged.at[panel_of(me, m)], inc[m].at[me],
                              local_sem.at[m]).wait()
        whole = pltpu.make_async_remote_copy(
            src_ref=inc[m].at[pl.ds(0, R - 1)], dst_ref=inc[m].at[pl.ds(0, R - 1)],
            send_sem=send_sem.at[m], recv_sem=recv_sem.at[m],
            device_id=(me, grp), device_id_type=MESH)
        whole.wait_send()
        whole.wait_recv()

    for m in range(1, M):
        send_all(m)

    @pl.when(grp != 0)
    def _():
        send_all(0)

    def source_of(g):
        def look(r, carry):
            end, behind, begin = carry
            end = end + counts_ref[r]
            past = g >= end
            return (end, behind + jnp.where(past, 1, 0), jnp.where(past, end, begin))

        zero = jnp.int32(0)
        _, source, begin = lax.fori_loop(0, R, look, (zero, zero, zero), unroll=R <= 8)
        return (jnp.minimum(source, R - 1) * (C + 1)
                + jnp.minimum(lax.div(g - begin, R), C - 1))

    for m in range(M):
        anchor = panel_of(me, m)

        def note(c, _):
            place[m, c] = source_of(c * R + anchor)
            return 0

        lax.fori_loop(0, DOC_DEV, note, 0)

    lane = lax.broadcasted_iota(jnp.int32, (1, T), 1)

    def landing(anchor, shift, height):
        def fill(r, carry):
            begin, line = carry
            count = counts_ref[r]
            b = lax.rem(anchor + R - lax.rem(begin, R), R)
            slot = (lane - r * C) * R + b
            good = (lane >= r * C) & (lane < r * C + C) & (slot < count)
            return begin + count, jnp.where(good, begin + slot, line)

        _, line = lax.fori_loop(0, R, fill, (jnp.int32(0), jnp.full((1, T), -(1 << 30), jnp.int32)),
                                unroll=R <= 8)
        rows = lax.broadcasted_iota(jnp.int32, (height, T), 0) - shift
        return jnp.where(rows * R + anchor == line, 1.0, 0.0).astype(jnp.bfloat16)

    def ids_of(m):
        def add(r, total):
            return total + inc[m][r, C].astype(jnp.float32)

        return lax.fori_loop(0, R, add, jnp.zeros((K, T), jnp.float32)).astype(jnp.bfloat16)

    def compact(m, dest, shift, stride):
        flat = inc[m]

        def bring(c, _):
            at = place[m, c]
            block = flat[lax.div(at, C + 1), lax.rem(at, C + 1)]
            work[pl.ds(pl.multiple_of(c * K, K), K), :] = block.astype(jnp.float32)
            return 0

        lax.fori_loop(0, DOC_DEV, bring, 0, unroll=8)
        total = jnp.zeros((DOC_DEV, T), jnp.float32)
        for k in range(K):
            rows = work[pl.ds(k, DOC_DEV, stride=K), :]
            total = total + rows * rows
            dest[pl.ds(k * stride + shift, DOC_DEV), :] = rows.astype(dest.dtype)
        return jnp.sum(total, axis=1, keepdims=True)

    along = (((1,), (1,)), ((), ()))

    @pl.when(grp != 0)
    def _():
        wait_all(0)

    def load_own(m):
        norm = compact(m, own, 0, DOC_DEV)
        ids = lax.dot_general(landing(me, 0, DOC_DEV), ids_of(m), along,
                              preferred_element_type=jnp.float32)
        for k in range(K):
            own_ids[k] = jnp.broadcast_to(ids[:, k:k + 1], (DOC_DEV, width))
        return norm

    @pl.when(grp == 0)
    def _():
        wait_all(1)
        own_ids[K] = jnp.broadcast_to(load_own(1), (DOC_DEV, width))

    @pl.when(grp != 0)
    def _():
        own_ids[K] = jnp.broadcast_to(load_own(0), (DOC_DEV, width))
        wait_all(1)

    for m in range(2, M):
        wait_all(m)
    own_norm = own_ids[K]

    for first in range(0, span, pair):
        norms = []
        ids = jnp.zeros((K, width), jnp.float32)
        for h in range(pair):
            m = 1 + first + h
            norms.append(compact(m, other, h * DOC_DEV, width))
            ids = ids + lax.dot_general(
                ids_of(m), landing(panel_of(me, m), h * DOC_DEV, width), along,
                preferred_element_type=jnp.float32)
        other_ids[...] = ids
        norm = jnp.broadcast_to(jnp.concatenate(norms, axis=0), (width, T)).T[:DOC_DEV]

        def step(kp, acc):
            block = other[pl.ds(pl.multiple_of(kp * 2 * width, 2 * width), 2 * width), :]
            lines = [other_ids[pl.ds(2 * kp + i, 1), :] for i in range(2)]
            for quarter in range(4):
                span_k = K // 4
                rows = own[quarter * span_k * DOC_DEV:(quarter + 1) * span_k * DOC_DEV, :]
                gram = lax.dot_general(rows, block, along, preferred_element_type=jnp.float32)
                for kk in range(span_k):
                    mine = own_ids[quarter * span_k + kk]
                    for i in range(2):
                        part = gram[kk * DOC_DEV:(kk + 1) * DOC_DEV, i * width:(i + 1) * width]
                        acc = acc + jnp.where(mine == lines[i], part, 0.0)
            return acc

        product = lax.fori_loop(0, K // 2, step, jnp.zeros((DOC_DEV, width), jnp.float32))
        out_ref[:, first * DOC_DEV:first * DOC_DEV + width] = product / (
            own_norm + norm - product)


def solution(mesh):
    R, G = mesh.shape["rows"], mesh.shape["grp"]
    span = R // G
    pair = 2 if span % 2 == 0 else 1

    def on_device(tile_values, tile_ids, doc_tiles, row_counts):
        cap, K, T = tile_values.shape
        C = (cap + R - 1) // R
        me = lax.axis_index("rows")
        ids = jnp.pad(tile_ids, ((0, C * R - cap), (0, 0))).astype(jnp.bfloat16)
        ids = ids.reshape(C, R, K).transpose(1, 2, 0)
        spread = jnp.tile(ids, (1, 1, R))
        spread = jnp.where(jnp.arange(R * C) // C == me, spread, jnp.zeros((), jnp.bfloat16))
        idblk = jnp.pad(spread, ((0, 0), (0, 0), (0, T - R * C)))
        vmem = pl.BlockSpec(memory_space=pltpu.VMEM)
        smem = pl.BlockSpec(memory_space=pltpu.SMEM)
        return pl.pallas_call(
            functools.partial(kernel, R, G),
            out_shape=jax.ShapeDtypeStruct((DOC_DEV, span * DOC_DEV), jnp.float32),
            in_specs=[smem, smem, vmem, vmem],
            out_specs=vmem,
            scratch_shapes=[
                pltpu.VMEM((R, C + 1, K, T), jnp.bfloat16),
                pltpu.SMEM((span + 1, DOC_DEV), jnp.int32),
                pltpu.VMEM((DOC_DEV * K, T), jnp.float32),
                pltpu.VMEM((DOC_DEV * K, T), jnp.bfloat16),
                pltpu.VMEM((pair * DOC_DEV * K, T), jnp.bfloat16),
                pltpu.VMEM((K + 1, DOC_DEV, pair * DOC_DEV), jnp.float32),
                pltpu.VMEM((K, pair * DOC_DEV), jnp.float32),
                pltpu.SemaphoreType.DMA((span + 1,)),
                pltpu.SemaphoreType.DMA((span + 1,)),
                pltpu.SemaphoreType.DMA((span + 1,)),
            ] + [pltpu.VMEM((R, C + 1, K, T), jnp.bfloat16)] * (span + 1),
            compiler_params=pltpu.CompilerParams(collective_id=0, has_side_effects=True),
        )(row_counts, doc_tiles, tile_values, idblk)

    placed = (P("rows", None, None), P("rows", None), P("rows"), P())
    return jax.shard_map(
        on_device, mesh=mesh, in_specs=placed, out_specs=P("rows", "grp"), check_vma=False
    )
```

```python
import functools

import jax
import jax.numpy as jnp
from jax import lax
from jax.experimental import pallas as pl
from jax.experimental.pallas import tpu as pltpu
from jax.sharding import PartitionSpec as P

MESH = pl.DeviceIdType.MESH
DOC_DEV = 64
ALONG = (((1,), (1,)), ((), ()))


def kernel(R, G, counts_ref, tiles_ref, vals_ref, idblk_ref, out_ref,
           staged, inc_own, inc_peer, place, work, own, own_ids, fold,
           send_sem, recv_sem, *others):
    cap, K, T = vals_ref.shape
    H = staged.shape[1] - 1
    C = (cap + R - 1) // R
    span = len(others)
    D = DOC_DEV
    me = lax.axis_index("rows")
    grp = lax.axis_index("grp")
    core = lax.rem(grp, 2)
    peer = grp + 1 - 2 * core

    barrier = pltpu.get_barrier_semaphore()

    def greet(d, _):
        pl.semaphore_signal(barrier, inc=1, device_id=(lax.rem(me + d, R), grp),
                            device_id_type=MESH)
        return 0

    lax.fori_loop(1, R, greet, 0)
    pl.semaphore_signal(barrier, inc=1, device_id=(me, peer), device_id_type=MESH)

    def add_up(r, total):
        return total + jnp.where(r < me, counts_ref[r], 0)

    start = lax.fori_loop(0, R, add_up, jnp.int32(0), unroll=R <= 8)
    tile_line = lax.broadcasted_iota(jnp.int32, (K, T), 0)

    def stage(j, _):
        b = lax.rem(j + R - lax.rem(start, R), R)
        for h in range(H):
            s = jnp.minimum((core * H + h) * R + b, cap - 1)
            block = vals_ref[s].astype(jnp.float32)
            block = jnp.where(tile_line < tiles_ref[s], block, 0.0)
            staged[j, h] = block.astype(staged.dtype)
        staged[j, H] = idblk_ref[b]
        return 0

    lax.fori_loop(0, R, stage, 0)
    pl.semaphore_wait(barrier, R)

    def deal(d, _):
        row = lax.rem(me + d, R)
        pltpu.make_async_remote_copy(
            src_ref=staged.at[row], dst_ref=inc_own.at[me],
            send_sem=send_sem.at[0], recv_sem=recv_sem.at[0],
            device_id=(row, grp), device_id_type=MESH).start()
        return 0

    lax.fori_loop(1, R, deal, 0)
    keep = pltpu.make_async_copy(staged.at[me], inc_own.at[me], recv_sem.at[2])
    keep.start()

    def source_of(g):
        def look(r, carry):
            end, behind, begin = carry
            end = end + counts_ref[r]
            past = g >= end
            return (end, behind + jnp.where(past, 1, 0), jnp.where(past, end, begin))

        zero = jnp.int32(0)
        _, source, begin = lax.fori_loop(0, R, look, (zero, zero, zero), unroll=R <= 8)
        return jnp.minimum(source, R - 1), jnp.minimum(lax.div(g - begin, R), C - 1)

    def note(c, _):
        source, a = source_of(c * R + me)
        place[0, c] = source
        place[1, c] = a
        return 0

    lax.fori_loop(0, D, note, 0)

    lane = lax.broadcasted_iota(jnp.int32, (1, T), 1)

    def fill(r, carry):
        begin, line = carry
        count = counts_ref[r]
        b = lax.rem(me + R - lax.rem(begin, R), R)
        slot = (lane - r * C) * R + b
        good = (lane >= r * C) & (lane < r * C + C) & (slot < count)
        return begin + count, jnp.where(good, begin + slot, line)

    nowhere = jnp.full((1, T), -(1 << 30), jnp.int32)
    _, line = lax.fori_loop(0, R, fill, (jnp.int32(0), nowhere), unroll=R <= 8)

    def landing(shift):
        rows = lax.broadcasted_iota(jnp.int32, (2 * D, T), 0) - shift
        return jnp.where(rows * R + me == line, 1.0, 0.0).astype(jnp.bfloat16)

    low, high = landing(0), landing(D)

    keep.wait()
    dealt = pltpu.make_async_remote_copy(
        src_ref=staged.at[pl.ds(0, R - 1)], dst_ref=inc_own.at[pl.ds(0, R - 1)],
        send_sem=send_sem.at[0], recv_sem=recv_sem.at[0],
        device_id=(me, peer), device_id_type=MESH)
    dealt.wait_recv()
    swap = pltpu.make_async_remote_copy(
        src_ref=inc_own, dst_ref=inc_peer,
        send_sem=send_sem.at[1], recv_sem=recv_sem.at[1],
        device_id=(me, peer), device_id_type=MESH)
    swap.start()

    def add_ids(r, total):
        return total + inc_own[r, H].astype(jnp.float32)

    ids = lax.fori_loop(0, R, add_ids, jnp.zeros((K, T), jnp.float32), unroll=R <= 8)
    ids = ids.astype(jnp.bfloat16)
    mine = lax.dot_general(low, ids, ALONG, preferred_element_type=jnp.float32)
    both = [lax.dot_general(ids, hot, ALONG, preferred_element_type=jnp.float32)
            for hot in (low, high)]
    lines = both[0][:K // 2] + both[1][K // 2:]
    own[K * D:K * D + K, :] = jnp.concatenate([lines, lines], axis=0).astype(own.dtype)
    for k in range(K):
        own_ids[k] = jnp.broadcast_to(mine[:D, k:k + 1], (D, T))
    swap.wait_recv()

    def bring(c, _):
        source, a = place[0, c], place[1, c]
        ours = lax.div(a, H) == core
        h = lax.rem(a, H)
        block = jnp.where(ours, inc_own[source, h].astype(jnp.float32),
                          inc_peer[source, h].astype(jnp.float32))
        work[pl.ds(pl.multiple_of(c * K, K), K), :] = block
        return 0

    lax.fori_loop(0, D, bring, 0, unroll=8)
    total = jnp.zeros((D, T), jnp.float32)
    for k in range(K):
        rows = work[pl.ds(k, D, stride=K), :]
        total = total + rows * rows
        own[k * D:(k + 1) * D, :] = rows.astype(own.dtype)
    own_norm = jnp.broadcast_to(jnp.sum(total, axis=1, keepdims=True), (D, T))

    def outgoing(i):
        return pltpu.make_async_remote_copy(
            src_ref=own, dst_ref=others[i],
            send_sem=send_sem.at[2 + i], recv_sem=recv_sem.at[3 + i],
            device_id=(lax.rem(me + grp * span + i, R), grp), device_id_type=MESH)

    first_copy = pltpu.make_async_copy(own, others[0], recv_sem.at[3])
    for i in range(1, span):
        outgoing(i).start()

    @pl.when(grp != 0)
    def _():
        outgoing(0).start()

    @pl.when(grp == 0)
    def _():
        first_copy.start()

    def compare(i):
        other = others[i]
        fold[...] = other[K * D:K * D + K, :].astype(jnp.float32)

        def norm_part(k, total):
            rows = other[pl.ds(pl.multiple_of(k * D, D), D), :].astype(jnp.float32)
            return total + rows * rows

        total = lax.fori_loop(0, K, norm_part, jnp.zeros((D, T), jnp.float32), unroll=4)
        total = jnp.broadcast_to(jnp.sum(total, axis=1, keepdims=True), (D, T))
        norm = jnp.concatenate([total, total], axis=0).T[:D]

        def step(p, acc):
            parts = [other[pl.ds(pl.multiple_of(k * D, D), D), :]
                     for k in (2 * p, 2 * p + K // 2, 2 * p + 1, 2 * p + 1 + K // 2)]
            block = jnp.concatenate(parts, axis=0)
            marks = [fold[pl.ds(2 * p + i, 1), :] for i in range(2)]
            some = K // 4
            for quarter in range(4):
                rows = own[quarter * some * D:(quarter + 1) * some * D, :]
                gram = lax.dot_general(rows, block, ALONG, preferred_element_type=jnp.float32)
                for kk in range(some):
                    here = own_ids[quarter * some + kk]
                    for i in range(2):
                        part = gram[kk * D:(kk + 1) * D, i * T:(i + 1) * T]
                        acc = acc + jnp.where(here == marks[i], part, 0.0)
            return acc

        acc = lax.fori_loop(0, K // 4, step, jnp.zeros((D, T), jnp.float32))
        product = acc[:, :D] + acc[:, D:2 * D]
        out_ref[:, i * D:(i + 1) * D] = product / (own_norm[:, :D] + norm[:, :D] - product)

    @pl.when(grp != 0)
    def _():
        outgoing(0).wait_recv()

    @pl.when(grp == 0)
    def _():
        first_copy.wait()

    compare(0)
    for i in range(1, span):
        outgoing(i).wait_recv()
        compare(i)

    dealt.wait_send()
    swap.wait_send()
    for i in range(1, span):
        outgoing(i).wait_send()

    @pl.when(grp != 0)
    def _():
        outgoing(0).wait_send()


def solution(mesh):
    R, G = mesh.shape["rows"], mesh.shape["grp"]
    span = R // G

    def on_device(tile_values, tile_ids, doc_tiles, row_counts):
        cap, K, T = tile_values.shape
        C = (cap + R - 1) // R
        H = (C + 1) // 2
        me = lax.axis_index("rows")
        ids = jnp.pad(tile_ids, ((0, C * R - cap), (0, 0))).astype(jnp.bfloat16)
        ids = ids.reshape(C, R, K).transpose(1, 2, 0)
        spread = jnp.tile(ids, (1, 1, R))
        spread = jnp.where(jnp.arange(R * C) // C == me, spread, jnp.zeros((), jnp.bfloat16))
        idblk = jnp.pad(spread, ((0, 0), (0, 0), (0, T - R * C)))
        vmem = pl.BlockSpec(memory_space=pltpu.VMEM)
        smem = pl.BlockSpec(memory_space=pltpu.SMEM)
        panel = pltpu.VMEM((DOC_DEV * K + K, T), jnp.bfloat16)
        return pl.pallas_call(
            functools.partial(kernel, R, G),
            out_shape=jax.ShapeDtypeStruct((DOC_DEV, span * DOC_DEV), jnp.float32),
            in_specs=[smem, smem, vmem, vmem],
            out_specs=vmem,
            scratch_shapes=[
                pltpu.VMEM((R, H + 1, K, T), jnp.bfloat16),
                pltpu.VMEM((R, H + 1, K, T), jnp.bfloat16),
                pltpu.VMEM((R, H + 1, K, T), jnp.bfloat16),
                pltpu.SMEM((2, DOC_DEV), jnp.int32),
                pltpu.VMEM((DOC_DEV * K, T), jnp.float32),
                panel,
                pltpu.VMEM((K, DOC_DEV, T), jnp.float32),
                pltpu.VMEM((K, T), jnp.float32),
                pltpu.SemaphoreType.DMA((span + 2,)),
                pltpu.SemaphoreType.DMA((span + 3,)),
            ] + [panel] * span,
            compiler_params=pltpu.CompilerParams(collective_id=0, has_side_effects=True),
        )(row_counts, doc_tiles, tile_values, idblk)

    placed = (P("rows", None, None), P("rows", None), P("rows"), P())
    return jax.shard_map(
        on_device, mesh=mesh, in_specs=placed, out_specs=P("rows", "grp"), check_vma=False
    )
```

```python
import functools

import jax
import jax.numpy as jnp
from jax import lax
from jax.experimental import pallas as pl
from jax.experimental.pallas import tpu as pltpu
from jax.sharding import PartitionSpec as P

MESH = pl.DeviceIdType.MESH
DOC_DEV = 64
ALONG = (((1,), (1,)), ((), ()))


def kernel(R, G, counts_ref, tiles_ref, vals_ref, idblk_ref, out_ref,
           staged, inc_own, inc_peer, place, work, own, own_ids, fold,
           vals, vals_sem, ahead, back, send_sem, recv_sem, give_sem, take_sem, *others):
    cap, K, T = vals_ref.shape
    H = staged.shape[1] - 1
    C = (cap + R - 1) // R
    span = len(others)
    D = DOC_DEV
    me = lax.axis_index("rows")
    grp = lax.axis_index("grp")
    core = lax.rem(grp, 2)
    peer = grp + 1 - 2 * core

    window = vals.shape[0]
    base = jnp.minimum(core * window, cap - window)
    fetch = pltpu.make_async_copy(vals_ref.at[pl.ds(base, window)], vals, vals_sem)
    fetch.start()
    barrier = pltpu.get_barrier_semaphore()

    def greet(d, _):
        pl.semaphore_signal(barrier, inc=1, device_id=(lax.rem(me + d, R), grp),
                            device_id_type=MESH)
        return 0

    lax.fori_loop(1, R, greet, 0)
    pl.semaphore_signal(barrier, inc=1, device_id=(me, peer), device_id_type=MESH)
    order = range(span - 1, -1, -1)

    def distance(i):
        return grp * span + i

    def formed(i):
        k = distance(i)
        return (k == 0) | ((k >= span) & (2 * k <= R)) | (k > R - span)

    def given(i):
        k = distance(i)
        return formed(i) & (k != 0) & (2 * k != R)

    for i in range(span):
        k = R - distance(i)

        @pl.when(jnp.logical_not(formed(i)))
        def _():
            pl.semaphore_signal(barrier, inc=1, device_id=(lax.rem(me + k, R), lax.div(k, span)),
                                device_id_type=MESH)

    def add_up(r, total):
        return total + jnp.where(r < me, counts_ref[r], 0)

    start = lax.fori_loop(0, R, add_up, jnp.int32(0), unroll=R <= 8)
    tile_line = lax.broadcasted_iota(jnp.int32, (K, T), 0)

    def stage(j, _):
        b = lax.rem(j + R - lax.rem(start, R), R)
        for h in range(H):
            s = jnp.minimum((core * H + h) * R + b, cap - 1)
            block = vals[s - base].astype(jnp.float32)
            block = jnp.where(tile_line < tiles_ref[s], block, 0.0)
            staged[j, h] = block.astype(staged.dtype)
        staged[j, H] = idblk_ref[b]
        return 0

    fetch.wait()
    lax.fori_loop(0, R, stage, 0)
    givers = sum(jnp.where(given(i), 1, 0) for i in range(span))
    pl.semaphore_wait(barrier, R + givers)

    def deal(d, _):
        row = lax.rem(me + d, R)
        pltpu.make_async_remote_copy(
            src_ref=staged.at[row], dst_ref=inc_own.at[me],
            send_sem=send_sem.at[0], recv_sem=recv_sem.at[0],
            device_id=(row, grp), device_id_type=MESH).start()
        return 0

    lax.fori_loop(1, R, deal, 0)
    keep = pltpu.make_async_copy(staged.at[me], inc_own.at[me], recv_sem.at[2])
    keep.start()

    def source_of(g):
        def look(r, carry):
            end, behind, begin = carry
            end = end + counts_ref[r]
            past = g >= end
            return (end, behind + jnp.where(past, 1, 0), jnp.where(past, end, begin))

        zero = jnp.int32(0)
        _, source, begin = lax.fori_loop(0, R, look, (zero, zero, zero), unroll=R <= 8)
        return jnp.minimum(source, R - 1), jnp.minimum(lax.div(g - begin, R), C - 1)

    def note(c, _):
        source, a = source_of(c * R + me)
        place[0, c] = source
        place[1, c] = a
        return 0

    lax.fori_loop(0, D, note, 0)

    lane = lax.broadcasted_iota(jnp.int32, (1, T), 1)

    def fill(r, carry):
        begin, line = carry
        count = counts_ref[r]
        b = lax.rem(me + R - lax.rem(begin, R), R)
        slot = (lane - r * C) * R + b
        good = (lane >= r * C) & (lane < r * C + C) & (slot < count)
        return begin + count, jnp.where(good, begin + slot, line)

    nowhere = jnp.full((1, T), -(1 << 30), jnp.int32)
    _, line = lax.fori_loop(0, R, fill, (jnp.int32(0), nowhere), unroll=R <= 8)

    def landing(shift):
        rows = lax.broadcasted_iota(jnp.int32, (2 * D, T), 0) - shift
        return jnp.where(rows * R + me == line, 1.0, 0.0).astype(jnp.bfloat16)

    low, high = landing(0), landing(D)

    keep.wait()
    dealt = pltpu.make_async_remote_copy(
        src_ref=staged.at[pl.ds(0, R - 1)], dst_ref=inc_own.at[pl.ds(0, R - 1)],
        send_sem=send_sem.at[0], recv_sem=recv_sem.at[0],
        device_id=(me, peer), device_id_type=MESH)
    dealt.wait_recv()
    swap = pltpu.make_async_remote_copy(
        src_ref=inc_own, dst_ref=inc_peer,
        send_sem=send_sem.at[1], recv_sem=recv_sem.at[1],
        device_id=(me, peer), device_id_type=MESH)
    swap.start()

    def add_ids(r, total):
        return total + inc_own[r, H].astype(jnp.float32)

    ids = lax.fori_loop(0, R, add_ids, jnp.zeros((K, T), jnp.float32), unroll=R <= 8)
    ids = ids.astype(jnp.bfloat16)
    mine = lax.dot_general(low, ids, ALONG, preferred_element_type=jnp.float32)
    both = [lax.dot_general(ids, hot, ALONG, preferred_element_type=jnp.float32)
            for hot in (low, high)]
    lines = both[0][:K // 2] + both[1][K // 2:]
    own[K * D:K * D + K, :] = jnp.concatenate([lines, lines], axis=0).astype(own.dtype)
    for k in range(K):
        own_ids[k] = jnp.broadcast_to(mine[:D, k:k + 1], (D, T))
    swap.wait_recv()

    def bring(c, _):
        source, a = place[0, c], place[1, c]
        ours = lax.div(a, H) == core
        h = lax.rem(a, H)
        block = jnp.where(ours, inc_own[source, h].astype(jnp.float32),
                          inc_peer[source, h].astype(jnp.float32))
        work[pl.ds(pl.multiple_of(c * K, K), K), :] = block
        return 0

    lax.fori_loop(0, D, bring, 0, unroll=8)
    total = jnp.zeros((D, T), jnp.float32)
    for k in range(K):
        rows = work[pl.ds(k, D, stride=K), :]
        total = total + rows * rows
        own[k * D:(k + 1) * D, :] = rows.astype(own.dtype)
    own_norm = jnp.broadcast_to(jnp.sum(total, axis=1, keepdims=True), (D, T))

    def outgoing(i):
        return pltpu.make_async_remote_copy(
            src_ref=own, dst_ref=others[i],
            send_sem=send_sem.at[2 + i], recv_sem=recv_sem.at[3 + i],
            device_id=(lax.rem(me + grp * span + i, R), grp), device_id_type=MESH)

    first_copy = pltpu.make_async_copy(own, others[0], recv_sem.at[3])

    def when_travels(i, act):
        k = distance(i)

        @pl.when((k != 0) & formed(i))
        def _():
            act(outgoing(i))

    for i in order:
        when_travels(i, lambda copy: copy.start())

    @pl.when(grp == 0)
    def _():
        first_copy.start()

    def giving(i):
        k = distance(i)
        twin = R - k
        j = (span - i) % span
        return pltpu.make_async_remote_copy(
            src_ref=ahead.at[i], dst_ref=back.at[j],
            send_sem=give_sem.at[i], recv_sem=take_sem.at[j],
            device_id=(lax.rem(me + twin, R), lax.div(twin, span)), device_id_type=MESH)

    def compare(i):
        other = others[i]
        fold[...] = other[K * D:K * D + K, :].astype(jnp.float32)

        def norm_part(k, total):
            rows = other[pl.ds(pl.multiple_of(k * D, D), D), :].astype(jnp.float32)
            return total + rows * rows

        total = lax.fori_loop(0, K, norm_part, jnp.zeros((D, T), jnp.float32), unroll=4)
        total = jnp.broadcast_to(jnp.sum(total, axis=1, keepdims=True), (D, T))
        norm = jnp.concatenate([total, total], axis=0).T[:D]

        def step(p, acc):
            parts = [other[pl.ds(pl.multiple_of(k * D, D), D), :]
                     for k in (2 * p, 2 * p + K // 2, 2 * p + 1, 2 * p + 1 + K // 2)]
            block = jnp.concatenate(parts, axis=0)
            marks = [fold[pl.ds(2 * p + i, 1), :] for i in range(2)]
            some = K // 4
            for quarter in range(4):
                rows = own[quarter * some * D:(quarter + 1) * some * D, :]
                gram = lax.dot_general(rows, block, ALONG, preferred_element_type=jnp.float32)
                for kk in range(some):
                    here = own_ids[quarter * some + kk]
                    for i in range(2):
                        part = gram[kk * D:(kk + 1) * D, i * T:(i + 1) * T]
                        acc = acc + jnp.where(here == marks[i], part, 0.0)
            return acc

        acc = lax.fori_loop(0, K // 4, step, jnp.zeros((D, T), jnp.float32))
        product = acc[:, :D] + acc[:, D:2 * D]
        block = product / (own_norm[:, :D] + norm[:, :D] - product)
        wide = jnp.concatenate([block, block], axis=1)
        ahead[i] = jnp.concatenate([wide, wide], axis=0).T[:D]
        out_ref[:, i * D:(i + 1) * D] = block

    for i in order:
        k = distance(i)
        if i == 0:
            @pl.when(grp == 0)
            def _():
                first_copy.wait()

        when_travels(i, lambda copy: copy.wait_recv())

        @pl.when(formed(i))
        def _():
            compare(i)

        @pl.when(given(i))
        def _():
            giving(i).start()

    for i in order:
        k = distance(i)

        @pl.when(jnp.logical_not(formed(i)))
        def _():
            pltpu.make_async_remote_copy(
                src_ref=ahead.at[i], dst_ref=back.at[i],
                send_sem=give_sem.at[i], recv_sem=take_sem.at[i],
                device_id=(me, peer), device_id_type=MESH).wait_recv()
            out_ref[:, i * D:(i + 1) * D] = back[i][:, :D]

        @pl.when(given(i))
        def _():
            giving(i).wait_send()

        when_travels(i, lambda copy: copy.wait_send())

    dealt.wait_send()
    swap.wait_send()


def solution(mesh):
    R, G = mesh.shape["rows"], mesh.shape["grp"]
    span = R // G

    def on_device(tile_values, tile_ids, doc_tiles, row_counts):
        cap, K, T = tile_values.shape
        C = (cap + R - 1) // R
        H = (C + 1) // 2
        me = lax.axis_index("rows")
        ids = jnp.pad(tile_ids, ((0, C * R - cap), (0, 0))).astype(jnp.bfloat16)
        ids = ids.reshape(C, R, K).transpose(1, 2, 0)
        spread = jnp.tile(ids, (1, 1, R))
        spread = jnp.where(jnp.arange(R * C) // C == me, spread, jnp.zeros((), jnp.bfloat16))
        idblk = jnp.pad(spread, ((0, 0), (0, 0), (0, T - R * C)))
        vmem = pl.BlockSpec(memory_space=pltpu.VMEM)
        smem = pl.BlockSpec(memory_space=pltpu.SMEM)
        panel = pltpu.VMEM((DOC_DEV * K + K, T), jnp.bfloat16)
        return pl.pallas_call(
            functools.partial(kernel, R, G),
            out_shape=jax.ShapeDtypeStruct((DOC_DEV, span * DOC_DEV), jnp.float32),
            in_specs=[smem, smem, pl.BlockSpec(memory_space=pl.ANY), vmem],
            out_specs=vmem,
            scratch_shapes=[
                pltpu.VMEM((R, H + 1, K, T), jnp.bfloat16),
                pltpu.VMEM((R, H + 1, K, T), jnp.bfloat16),
                pltpu.VMEM((R, H + 1, K, T), jnp.bfloat16),
                pltpu.SMEM((2, DOC_DEV), jnp.int32),
                pltpu.VMEM((DOC_DEV * K, T), jnp.float32),
                panel,
                pltpu.VMEM((K, DOC_DEV, T), jnp.float32),
                pltpu.VMEM((K, T), jnp.float32),
                pltpu.VMEM((min(H * R, cap), K, T), jnp.bfloat16),
                pltpu.SemaphoreType.DMA,
                pltpu.VMEM((span, DOC_DEV, T), jnp.float32),
                pltpu.VMEM((span, DOC_DEV, T), jnp.float32),
                pltpu.SemaphoreType.DMA((span + 2,)),
                pltpu.SemaphoreType.DMA((span + 3,)),
                pltpu.SemaphoreType.DMA((span,)),
                pltpu.SemaphoreType.DMA((span,)),
            ] + [panel] * span,
            compiler_params=pltpu.CompilerParams(collective_id=0, has_side_effects=True),
        )(row_counts, doc_tiles, tile_values, idblk)

    placed = (P("rows", None, None), P("rows", None), P("rows"), P())
    return jax.shard_map(
        on_device, mesh=mesh, in_specs=placed, out_specs=P("rows", "grp"), check_vma=False
    )
```
